32 devices in a mesh: ta: 16 (over z, y, x), sa: 2 (over core).
Axes of the slice: x: 2, y: 2, z: 4, core: 2. Of those that a mesh axis runs over, the one named last changes fastest.
Arguments:
- rhs: float32 [1, 2, 40, 16, 2, 128], P(None, None, None, 'ta', 'sa'), may hold values from -6 to 6
- links: bfloat16 [4, 2, 40, 40, 16, 2, 128], P(None, None, None, None, 'ta', 'sa'), may hold values from -0.625 to 0.625
- clover: bfloat16 [2, 40, 40, 16, 2, 128], P(None, None, None, 'ta', 'sa'), may hold values from -1 to 7
- mr_steps: int32 [16, 2, 2], P('ta', 'sa'), may hold values from 2 to 3
Outputs:
- solution: float32 [1, 2, 40, 16, 2, 128], P(None, None, None, 'ta', 'sa')
- residual: float32 [1, 2, 40, 16, 2, 128], P(None, None, None, 'ta', 'sa')
The draws below stay inside these ranges and needn't reach their ends.
All inputs are finite; a program needn't handle non-finite values.
Results may differ from the reference program's by a relative error of at most 0.0003.
Values sent between devices are 32-bit elements; how exact they have to be, the bound alone decides.
A program may use at most 128 MiB of HBM per device.

```python
import jax
import jax.numpy as jnp
from jax import lax

NVEC = 20
DOF = 40
NRHS = 1
TD = 2
LZ = 4
LY = 4
LX = 4
MR_MAX = 3
SWEEPS = 2
NTD = 16
NZD = 2
DS = 128


def draw_clover(key, part):
    folded = jax.random.fold_in(key, 7)
    first, second = jax.random.split(folded)
    shape = (2, DOF, DOF, NTD, NZD, DS)
    spread = jax.random.normal(first, shape, jnp.float32) / jnp.sqrt(jnp.float32(DOF))
    diagonal = jax.random.uniform(second, (NTD, NZD, DS), jnp.float32, 3.5, 5.0)
    spread = jnp.clip(spread, -1.0, 1.0)
    identity = jnp.eye(DOF, dtype=jnp.float32)[:, :, None, None, None]
    real_part = spread[0] + identity * diagonal[None, None]
    return jnp.stack([real_part, spread[1]], 0).astype(jnp.bfloat16)


def with_ends(array, rng, low, largest):
    spot = [jax.random.randint(jax.random.fold_in(rng, axis), (), 0, length) for axis, length in enumerate(array.shape)]
    longest = array.shape.index(max(array.shape))
    neighbour = spot[:longest] + [(spot[longest] + 1) % array.shape[longest]] + spot[longest + 1:]
    return array.at[tuple(spot)].set(low).at[tuple(neighbour)].set(largest)


def levels(own_key, shape, cuts, smallest, top_value):
    factor_of = 1.0
    for axis_at, shards_of in cuts:
        draws = jax.random.uniform(jax.random.fold_in(jax.random.fold_in(own_key, 6), axis_at), (shards_of,), jnp.float32, smallest / len(cuts), top_value / len(cuts))
        factor_of = factor_of * jnp.repeat(jnp.exp(draws), shape[axis_at] // shards_of).reshape((-1,) + (1,) * (len(shape) - 1 - axis_at))
    return factor_of


def bell_draw(own_key, shape, deviation, most, cuts=(), kind=jnp.bfloat16):
    values = deviation * jax.random.normal(own_key, shape, jnp.float32)
    if cuts:
        values = values * levels(own_key, shape, cuts, -0.22, 0.18)
    return jnp.clip(values, -most, most).astype(kind)


def setup_inputs(seed: int = 0) -> dict:
    key_list = jax.random.split(jax.random.key(seed), 5)
    rhs = bell_draw(key_list[0], (NRHS, 2, DOF, NTD, NZD, DS), 1.0, 6.0, ((3, 16), (4, 2)), jnp.float32)
    links = bell_draw(key_list[1], (4, 2, DOF, DOF, NTD, NZD, DS), (2 * DOF) ** -0.5, 0.625, ((4, 16), (5, 2)))
    clover = draw_clover(jax.random.fold_in(key_list[4], 71), 0)
    mr_steps = with_ends(jax.random.randint(key_list[3], (NTD, NZD, 2), 2, MR_MAX + 1), jax.random.fold_in(key_list[3], 1), 2, MR_MAX).astype(jnp.int32)
    return {"rhs": rhs, "links": links, "clover": clover, "mr_steps": mr_steps}


HIGHEST = lax.Precision.HIGHEST


def complex_apply(matrices, vectors, dagger):
    real_mat = matrices[0].astype(jnp.float32)
    imag_mat = matrices[1].astype(jnp.float32)
    real_vec = vectors[:, 0]
    imag_vec = vectors[:, 1]
    pattern = "ji...,rj...->ri..." if dagger else "ij...,rj...->ri..."

    def product(left, right):
        return jnp.einsum(pattern, left, right, precision=HIGHEST)

    if dagger:
        real_out = product(real_mat, real_vec) + product(imag_mat, imag_vec)
        imag_out = product(real_mat, imag_vec) - product(imag_mat, real_vec)
    else:
        real_out = product(real_mat, real_vec) - product(imag_mat, imag_vec)
        imag_out = product(real_mat, imag_vec) + product(imag_mat, real_vec)
    return jnp.stack([real_out, imag_out], axis=1)


def lattice_view(field):
    leading = field.shape[:3]
    shaped = field.reshape(leading + (NTD, NZD, TD, LZ, LY, LX))
    shaped = jnp.transpose(shaped, (0, 1, 2, 3, 5, 4, 6, 7, 8))
    return shaped.reshape(leading + (NTD * TD, NZD * LZ, LY, LX))


def domain_view(lattice):
    leading = lattice.shape[:3]
    shaped = lattice.reshape(leading + (NTD, TD, NZD, LZ, LY, LX))
    shaped = jnp.transpose(shaped, (0, 1, 2, 3, 5, 4, 6, 7, 8))
    return shaped.reshape(leading + (NTD, NZD, DS))


def shifted(field, direction, amount):
    return domain_view(jnp.roll(lattice_view(field), amount, axis=3 + direction))


def apply_operator(field, links, clover):
    signs = jnp.where(jnp.arange(DOF) < NVEC, 1.0, -1.0).astype(jnp.float32)[:, None, None]

    def backward_terms(index):
        vectors = lax.dynamic_index_in_dim(field, index, 3, keepdims=False)
        matrices = lax.dynamic_index_in_dim(links, index, 4, keepdims=False)
        return jnp.stack([signs * complex_apply(matrices[direction], signs * vectors, True) for direction in range(4)], 0)

    back_terms = jnp.moveaxis(lax.map(backward_terms, jnp.arange(NTD)), 0, 4)
    neighbours = jnp.stack([shifted(field, direction, -1) for direction in range(4)], 0)
    behind_total = shifted(back_terms[0], 0, 1)
    for direction in range(1, 4):
        behind_total = behind_total + shifted(back_terms[direction], direction, 1)

    def forward_terms(index):
        vectors = lax.dynamic_index_in_dim(field, index, 3, keepdims=False)
        nearby = lax.dynamic_index_in_dim(neighbours, index, 4, keepdims=False)
        matrices = lax.dynamic_index_in_dim(links, index, 4, keepdims=False)
        self_block = lax.dynamic_index_in_dim(clover, index, 3, keepdims=False)
        total = complex_apply(self_block, vectors, False)
        for direction in range(4):
            total = total - complex_apply(matrices[direction], nearby[direction], False)
        return total

    result = jnp.moveaxis(lax.map(forward_terms, jnp.arange(NTD)), 0, 3)
    return result - behind_total


def block_sums(component):
    shaped = component.reshape(component.shape[:4] + (2, DS // 2))
    return jnp.sum(shaped, axis=(1, 5))


def block_scale(factor, component):
    shaped = component.reshape(component.shape[:4] + (2, DS // 2))
    return (factor[:, None, :, :, :, None] * shaped).reshape(component.shape)


def reference(rhs, links, clover, mr_steps):
    colour = (jnp.arange(DS)[None, :] // (DS // 2) + jnp.arange(NZD)[:, None]) % 2
    solution = jnp.zeros_like(rhs)
    for sweep_index in range(SWEEPS):
        for colour_index in range(2):
            mask = (colour == colour_index).astype(jnp.float32)
            remainder = rhs - apply_operator(solution, links, clover)
            search = remainder * mask
            correction = jnp.zeros_like(search)
            for step_index in range(MR_MAX):
                image = apply_operator(search, links, clover) * mask
                real_s = search[:, 0]
                imag_s = search[:, 1]
                real_q = image[:, 0]
                imag_q = image[:, 1]
                numer_real = block_sums(real_q * real_s + imag_q * imag_s)
                numer_imag = block_sums(real_q * imag_s - imag_q * real_s)
                denom = block_sums(real_q * real_q + imag_q * imag_q) + 1e-6
                live = (step_index < mr_steps)[None]
                alpha_real = jnp.where(live, numer_real / denom, 0.0)
                alpha_imag = jnp.where(live, numer_imag / denom, 0.0)
                correction = correction + jnp.stack([block_scale(alpha_real, real_s) - block_scale(alpha_imag, imag_s), block_scale(alpha_real, imag_s) + block_scale(alpha_imag, real_s)], 1)
                search = search - jnp.stack([block_scale(alpha_real, real_q) - block_scale(alpha_imag, imag_q), block_scale(alpha_real, imag_q) + block_scale(alpha_imag, real_q)], 1)
            solution = solution + correction
    residual = rhs - apply_operator(solution, links, clover)
    return solution, residual
```

```python
import functools

import jax
import jax.numpy as jnp
from jax import lax
from jax.experimental import pallas as pl
from jax.experimental.pallas import tpu as pltpu
from jax.sharding import PartitionSpec as P

LZ = 4
LY = 4
LX = 4
MR_MAX = 3
SWEEPS = 2
PHASES = 2 * SWEEPS
UNROLL = 4
MESH = pl.DeviceIdType.MESH


def kernel(
    nt,
    nz,
    rhs_ref,
    links_ref,
    clover_ref,
    steps_ref,
    x_ref,
    r_ref,
    lk,
    cl,
    g,
    rs,
    xs,
    s_ref,
    e_ref,
    acc,
    gv,
    f_ref,
    sbuf,
    rbuf,
    csem,
    ssem,
    rsem,
):
    dof, lanes = rhs_ref.shape[1:]
    half = lanes // 2
    tiles = dof // 8
    ta = lax.axis_index("ta")
    sa = lax.axis_index("sa")
    t_next, t_prev = lax.rem(ta + 1, nt), lax.rem(ta + nt - 1, nt)
    z_next, z_prev = lax.rem(sa + 1, nz), lax.rem(sa + nz - 1, nz)

    copies = [
        pltpu.make_async_copy(links_ref.at[d], lk.at[d], csem.at[d]) for d in range(4)
    ] + [pltpu.make_async_copy(clover_ref, cl, csem.at[4])]
    for d in (2, 1, 3, 4, 0):
        copies[d].start()

    barrier = pltpu.get_barrier_semaphore()
    for where_to in ({"ta": t_next}, {"ta": t_prev}, {"sa": z_next}, {"sa": z_prev}):
        pl.semaphore_signal(barrier, inc=1, device_id=where_to, device_id_type=MESH)

    shape = (dof, lanes)
    lane = lax.broadcasted_iota(jnp.int32, shape, 1)
    row = lax.broadcasted_iota(jnp.int32, shape, 0)
    signs = jnp.where(row < dof // 2, 1.0, -1.0).astype(jnp.float32)
    low = lane < half
    site = lane % half
    zpos = site // (LY * LX)
    ypos = site // LX % LY
    xpos = site % LX
    z_last, z_first = zpos == LZ - 1, zpos == 0
    y_last, y_first = ypos == LY - 1, ypos == 0
    x_last, x_first = xpos == LX - 1, xpos == 0
    zero = jnp.zeros(shape, jnp.float32)
    plane = LY * LX

    def roll(v, by):
        return pltpu.roll(v, by % lanes, 1)

    for c in range(2):
        v = rhs_ref[c]
        w = roll(v, half)
        rs[0, c] = jnp.where(low, v, w)
        rs[1, c] = jnp.where(low, w, v)
        xs[0, c] = zero
        xs[1, c] = zero

    def prepare(plain, rolled, groups):
        def body(i, carry):
            for c in range(2):
                b = roll(rolled(c, i).astype(jnp.float32), half)
                for source, group in zip(plain, groups):
                    a = source(c, i).astype(jnp.float32)
                    g[group, 0, c, i] = jnp.where(low, a, b)
                    g[group, 1, c, i] = jnp.where(low, b, a)
            return carry

        lax.fori_loop(0, dof, body, 0)

    def link(d):
        return lambda c, i: lk[d, c, i]

    copies[2].wait()
    copies[1].wait()
    prepare([link(2)], link(1), [0])
    copies[3].wait()
    copies[4].wait()
    copies[0].wait()
    prepare([lambda c, i: cl[c, i], link(0)], link(3), [1, 2])
    prepare([link(0)], link(1), [3])

    def fold(v):
        total = v[0:8]
        for t in range(1, tiles):
            total = total + v[8 * t : 8 * t + 8]
        return total

    def gathered(slots):
        parts = []
        for t in range(tiles):
            total = None
            for slot in slots:
                for k in range(8):
                    piece = f_ref[slot, pl.ds(8 * 8 * t + k, 8, stride=8), :]
                    total = piece if total is None else total + piece
            parts.append(total)
        return jnp.concatenate(parts, axis=0)

    def sweep_matrices(forward, forward_half, inputs, backward, backward_half, slot):
        vr, vi = inputs
        vs = vr + vi
        shared = backward == forward

        def one(i, carry):
            mr, mi = g[forward, forward_half, 0, i], g[forward, forward_half, 1, i]
            ms = mr + mi
            p1 = fold(mr * vr)
            p2 = fold(mi * vi)
            p3 = fold(ms * vs)
            at = pl.multiple_of(8 * i, 8)
            f_ref[slot, pl.ds(at, 8), :] = p1 - p2
            f_ref[slot + 1, pl.ds(at, 8), :] = p3 - p1 - p2
            if backward is None:
                return carry
            if not shared:
                mr, mi = g[backward, backward_half, 0, i], g[backward, backward_half, 1, i]
                ms = mr + mi
            b1, b2, b3 = carry
            br = gv[0, pl.ds(i, 1), :]
            bi = gv[1, pl.ds(i, 1), :]
            bd = gv[2, pl.ds(i, 1), :]
            return (b1 + mr * br, b2 + mi * bi, b3 + ms * bd)

        def body(outer, carry):
            for inner in range(UNROLL):
                carry = one(outer * UNROLL + inner, carry)
            return carry

        start = 0 if backward is None else (zero, zero, zero)
        got = lax.fori_loop(0, dof // UNROLL, body, start)
        if backward is None:
            return None
        b1, b2, b3 = got
        return -signs * (b1 + b2), -signs * (b1 - b2 - b3)

    def phase(ph, token):
        h = lax.rem(ph + sa, 2)
        other = 1 - h
        limit = steps_ref[h]
        first = (lane // half) == h
        h_is_0 = (lane * 0 + h) == 0

        for c in range(2):
            s_ref[c] = rs[h, c]
            e_ref[c] = zero
            acc[0, c] = zero
            acc[1, c] = zero

        def step(k, carry):
            sr, si = s_ref[0], s_ref[1]
            gr, gi = signs * sr, signs * si
            gv[0] = gr
            gv[1] = gi
            gv[2] = gr - gi

            def ahead0(v):
                n = -v
                ya = jnp.where(y_last, roll(n, (LY - 1) * LX), roll(n, -LX))
                za = jnp.where(z_last, 0.0, roll(n, -plane))
                return jnp.where(first, ya, za)

            def ahead1(v):
                n = -v
                xa = jnp.where(x_last, roll(n, LX - 1), roll(n, -1))
                return jnp.where(first, v, xa)

            back0 = sweep_matrices(0, h, (ahead0(sr), ahead0(si)), 0, h, 0)
            back2 = sweep_matrices(1, h, (ahead1(sr), ahead1(si)), 2, h, 2)
            q = []
            for c in range(2):
                b, d = back0[c], back2[c]
                yb = jnp.where(y_first, roll(b, -(LY - 1) * LX), roll(b, LX))
                zb = jnp.where(z_first, 0.0, roll(b, plane))
                xb = jnp.where(x_first, roll(d, -(LX - 1)), roll(d, 1))
                u = gathered((c, 2 + c)) + jnp.where(first, yb, zb) + jnp.where(first, 0.0, xb)
                q.append(u + roll(u, half))
            qr, qi = q

            def total(v):
                return jnp.sum(jnp.sum(fold(v), axis=0, keepdims=True), axis=1, keepdims=True)

            numer_real = total(qr * sr + qi * si)
            numer_imag = total(qr * si - qi * sr)
            denom = total(qr * qr + qi * qi) + 2e-6
            live = (lane * 0 + limit) > k
            ar = jnp.where(live, jnp.broadcast_to(numer_real / denom, shape), 0.0)
            ai = jnp.where(live, jnp.broadcast_to(numer_imag / denom, shape), 0.0)
            e_ref[0] += ar * sr - ai * si
            e_ref[1] += ar * si + ai * sr
            s_ref[0] = sr - (ar * qr - ai * qi)
            s_ref[1] = si - (ar * qi + ai * qr)
            for n, (vr, vi) in enumerate((back0, back2)):
                acc[n, 0] += ar * vr - ai * vi
                acc[n, 1] += ar * vi + ai * vr
            return carry

        lax.fori_loop(0, MR_MAX, step, 0)

        er, ei = e_ref[0], e_ref[1]
        bz = [-jnp.where(first, roll(acc[0, c], half), acc[0, c]) for c in range(2)]
        bt = [-jnp.where(first, acc[1, c], roll(acc[1, c], half)) for c in range(2)]
        packed = jnp.where(low, er, ei)
        sbuf[ph, 0] = jnp.where(h_is_0, packed, jnp.where(low, bt[0], bt[1]))
        sbuf[ph, 1] = packed
        sbuf[ph, 2] = jnp.where(low, bz[0], bz[1])

        @pl.when(ph == 0)
        def _():
            pl.semaphore_wait(barrier, 4)

        target = lax.rem(ta + nt + 2 * h - 1, nt)
        sends = []
        for n, where_to in enumerate(({"ta": target}, {"sa": z_prev}, {"sa": z_next})):
            send = pltpu.make_async_remote_copy(
                src_ref=sbuf.at[ph, n],
                dst_ref=rbuf.at[ph, n],
                send_sem=ssem.at[ph, n],
                recv_sem=rsem.at[ph, n],
                device_id=where_to,
                device_id_type=MESH,
            )
            send.start()
            sends.append(send)

        for c, ec in enumerate((er, ei)):
            xs[h, c] += ec
            rs[h, c] = s_ref[c]

        for send in sends:
            send.wait()

        def unpack(n):
            m = rbuf[ph, n]
            w = roll(m, half)
            return jnp.where(low, m, w), jnp.where(low, w, m)

        got_t, got_e, got_b = unpack(0), unpack(1), unpack(2)
        inputs = []
        for c, ec in enumerate((er, ei)):
            tin = jnp.where(h_is_0, got_t[c], ec)
            zin = jnp.where(z_last, roll(got_e[c], -plane), 0.0)
            inputs.append(jnp.where(first, zin, tin))
        sweep_matrices(3, other, inputs, None, None, 0)
        for c in range(2):
            u = gathered((c,))
            behind = jnp.where(h_is_0, bt[c], got_t[c])
            zb = jnp.where(z_first, roll(got_b[c], plane), 0.0)
            rs[other, c] += u + roll(u, half) + behind + zb
        return token

    lax.fori_loop(0, PHASES, phase, 0)

    for c in range(2):
        x_ref[c] = jnp.where(low, xs[0, c], xs[1, c])
        r_ref[c] = jnp.where(low, rs[0, c], rs[1, c])


def shards(nt, nz, rhs, links, clover, mr_steps):
    dof, lanes = rhs.shape[2], rhs.shape[-1]
    f32 = jnp.float32
    vmem = pl.BlockSpec(memory_space=pltpu.VMEM)
    hbm = pl.BlockSpec(memory_space=pl.ANY)
    x, r = pl.pallas_call(
        functools.partial(kernel, nt, nz),
        out_shape=[jax.ShapeDtypeStruct((2, dof, lanes), f32)] * 2,
        in_specs=[vmem, hbm, hbm, pl.BlockSpec(memory_space=pltpu.SMEM)],
        out_specs=[vmem, vmem],
        scratch_shapes=[
            pltpu.VMEM((4, 2, dof, dof, lanes), jnp.bfloat16),
            pltpu.VMEM((2, dof, dof, lanes), jnp.bfloat16),
            pltpu.VMEM((4, 2, 2, dof, dof, lanes), f32),
            pltpu.VMEM((2, 2, dof, lanes), f32),
            pltpu.VMEM((2, 2, dof, lanes), f32),
            pltpu.VMEM((2, dof, lanes), f32),
            pltpu.VMEM((2, dof, lanes), f32),
            pltpu.VMEM((2, 2, dof, lanes), f32),
            pltpu.VMEM((3, dof, lanes), f32),
            pltpu.VMEM((4, 8 * dof, lanes), f32),
            pltpu.VMEM((PHASES, 3, dof, lanes), f32),
            pltpu.VMEM((PHASES, 3, dof, lanes), f32),
            pltpu.SemaphoreType.DMA((5,)),
            pltpu.SemaphoreType.DMA((PHASES, 3)),
            pltpu.SemaphoreType.DMA((PHASES, 3)),
        ],
        compiler_params=pltpu.CompilerParams(
            collective_id=0, has_side_effects=True, vmem_limit_bytes=48 * 1024 * 1024
        ),
    )(
        rhs.reshape(2, dof, lanes),
        links.reshape(4, 2, dof, dof, lanes),
        clover.reshape(2, dof, dof, lanes),
        mr_steps.reshape(2),
    )
    return x.reshape(rhs.shape), r.reshape(rhs.shape)


def solution(mesh):
    placed = (
        P(None, None, None, "ta", "sa", None),
        P(None, None, None, None, "ta", "sa", None),
        P(None, None, None, "ta", "sa", None),
        P("ta", "sa", None),
    )
    return jax.shard_map(
        functools.partial(shards, mesh.shape["ta"], mesh.shape["sa"]),
        mesh=mesh,
        in_specs=placed,
        out_specs=(P(None, None, None, "ta", "sa", None), P(None, None, None, "ta", "sa", None)),
        check_vma=False,
    )
```

```python
import functools

import jax
import jax.numpy as jnp
from jax import lax
from jax.experimental import pallas as pl
from jax.experimental.pallas import tpu as pltpu
from jax.sharding import PartitionSpec as P

LZ = 4
LY = 4
LX = 4
MR_MAX = 3
SWEEPS = 2
PHASES = 2 * SWEEPS
UNROLL = 4
PREPARE_UNROLL = 8
MESH = pl.DeviceIdType.MESH


def kernel(
    nt,
    nz,
    rhs_hbm,
    links_ref,
    clover_ref,
    steps_hbm,
    x_ref,
    r_ref,
    rhs_ref,
    steps_ref,
    lk,
    cl,
    g,
    rs,
    xs,
    s_ref,
    e_ref,
    acc,
    a_ref,
    gv,
    f_ref,
    sbuf,
    rbuf,
    csem,
    ssem,
    rsem,
):
    dof, lanes = rhs_ref.shape[1:]
    half = lanes // 2
    tiles = dof // 8
    ta = lax.axis_index("ta")
    sa = lax.axis_index("sa")
    t_next, t_prev = lax.rem(ta + 1, nt), lax.rem(ta + nt - 1, nt)
    z_next, z_prev = lax.rem(sa + 1, nz), lax.rem(sa + nz - 1, nz)

    copies = [
        pltpu.make_async_copy(links_ref.at[d], lk.at[d], csem.at[d]) for d in range(4)
    ] + [
        pltpu.make_async_copy(clover_ref, cl, csem.at[4]),
        pltpu.make_async_copy(rhs_hbm, rhs_ref, csem.at[5]),
        pltpu.make_async_copy(steps_hbm, steps_ref, csem.at[6]),
    ]
    for d in (5, 1, 2, 0, 3, 4, 6):
        copies[d].start()

    barrier = pltpu.get_barrier_semaphore()
    for where_to in ({"ta": t_next}, {"ta": t_prev}, {"sa": z_next}, {"sa": z_prev}):
        pl.semaphore_signal(barrier, inc=1, device_id=where_to, device_id_type=MESH)

    shape = (dof, lanes)
    lane = lax.broadcasted_iota(jnp.int32, shape, 1)
    row = lax.broadcasted_iota(jnp.int32, shape, 0)
    signs = jnp.where(row < dof // 2, 1.0, -1.0).astype(jnp.float32)
    low = lane < half
    site = lane % half
    zpos = site // (LY * LX)
    ypos = site // LX % LY
    xpos = site % LX
    z_last, z_first = zpos == LZ - 1, zpos == 0
    y_last, y_first = ypos == LY - 1, ypos == 0
    x_last, x_first = xpos == LX - 1, xpos == 0
    zero = jnp.zeros(shape, jnp.float32)
    plane = LY * LX

    def roll(v, by):
        return pltpu.roll(v, by % lanes, 1)

    copies[5].wait()
    for c in range(2):
        v = rhs_ref[c]
        w = roll(v, half)
        rs[0, c] = jnp.where(low, v, w)
        rs[1, c] = jnp.where(low, w, v)
        xs[0, c] = zero
        xs[1, c] = zero

    def prepare(plain, rolled, groups):
        def body(outer, carry):
            for inner in range(PREPARE_UNROLL):
                i = outer * PREPARE_UNROLL + inner
                for c in range(2):
                    b = roll(rolled(c, i).astype(jnp.float32), half)
                    for source, group in zip(plain, groups):
                        a = source(c, i).astype(jnp.float32)
                        g[group, 0, c, i] = jnp.where(low, a, b)
                        g[group, 1, c, i] = jnp.where(low, b, a)
            return carry

        lax.fori_loop(0, dof // PREPARE_UNROLL, body, 0)

    def link(d):
        return lambda c, i: lk[d, c, i]

    for d in (1, 2, 0):
        copies[d].wait()
    prepare([link(2), link(0)], link(1), [0, 3])
    for d in (3, 4, 6):
        copies[d].wait()
    prepare([lambda c, i: cl[c, i], link(0)], link(3), [1, 2])

    def fold(v):
        total = v[0:8]
        for t in range(1, tiles):
            total = total + v[8 * t : 8 * t + 8]
        return total

    def gathered(slot):
        parts = []
        for t in range(tiles):
            total = None
            for k in range(8):
                piece = f_ref[slot, pl.ds(8 * 8 * t + k, 8, stride=8), :]
                total = piece if total is None else total + piece
            parts.append(total)
        return jnp.concatenate(parts, axis=0)

    def sweep_matrices(forward, forward_half, inputs, backward, backward_half, more):
        vr, vi = inputs
        vs = vr + vi
        shared = backward == forward

        def one(i, carry):
            mr, mi = g[forward, forward_half, 0, i], g[forward, forward_half, 1, i]
            ms = mr + mi
            p1 = fold(mr * vr)
            p2 = fold(mi * vi)
            p3 = fold(ms * vs)
            at = pl.multiple_of(8 * i, 8)
            real_part, imag_part = p1 - p2, p3 - p1 - p2
            if more:
                real_part = real_part + f_ref[0, pl.ds(at, 8), :]
                imag_part = imag_part + f_ref[1, pl.ds(at, 8), :]
            f_ref[0, pl.ds(at, 8), :] = real_part
            f_ref[1, pl.ds(at, 8), :] = imag_part
            if backward is None:
                return carry
            if not shared:
                mr, mi = g[backward, backward_half, 0, i], g[backward, backward_half, 1, i]
                ms = mr + mi
            b1, b2, b3 = carry
            br = gv[0, pl.ds(i, 1), :]
            bi = gv[1, pl.ds(i, 1), :]
            bd = gv[2, pl.ds(i, 1), :]
            return (b1 + mr * br, b2 + mi * bi, b3 + ms * bd)

        def body(outer, carry):
            for inner in range(UNROLL):
                carry = one(outer * UNROLL + inner, carry)
            return carry

        start = 0 if backward is None else (zero, zero, zero)
        got = lax.fori_loop(0, dof // UNROLL, body, start)
        if backward is None:
            return None
        b1, b2, b3 = got
        return -signs * (b1 + b2), -signs * (b1 - b2 - b3)

    def phase(ph, token):
        h = lax.rem(ph + sa, 2)
        other = 1 - h
        limit = steps_ref[h]
        first = (lane // half) == h
        h_is_0 = (lane * 0 + h) == 0

        def ahead(v):
            n = -v
            ya = jnp.where(y_last, roll(n, (LY - 1) * LX), roll(n, -LX))
            za = jnp.where(z_last, 0.0, roll(n, -plane))
            xa = jnp.where(x_last, roll(n, LX - 1), roll(n, -1))
            return jnp.where(first, ya, za), jnp.where(first, v, xa)

        for c in range(2):
            v = rs[h, c]
            s_ref[c] = v
            e_ref[c] = zero
            acc[0, c] = zero
            acc[1, c] = zero
            a_ref[0, c], a_ref[1, c] = ahead(v)

        def step(k, carry):
            sr, si = s_ref[0], s_ref[1]
            gr, gi = signs * sr, signs * si
            gv[0] = gr
            gv[1] = gi
            gv[2] = gr - gi
            back0 = sweep_matrices(0, h, (a_ref[0, 0], a_ref[0, 1]), 0, h, False)
            back2 = sweep_matrices(1, h, (a_ref[1, 0], a_ref[1, 1]), 2, h, True)
            q = []
            for c in range(2):
                b, d = back0[c], back2[c]
                yb = jnp.where(y_first, roll(b, -(LY - 1) * LX), roll(b, LX))
                zb = jnp.where(z_first, 0.0, roll(b, plane))
                xb = jnp.where(x_first, roll(d, -(LX - 1)), roll(d, 1))
                u = gathered(c) + jnp.where(first, yb, zb) + jnp.where(first, 0.0, xb)
                q.append(u + roll(u, half))
            qr, qi = q
            ahead_r, ahead_i = ahead(qr), ahead(qi)

            def total(v):
                return jnp.sum(jnp.sum(fold(v), axis=0, keepdims=True), axis=1, keepdims=True)

            numer_real = total(qr * sr + qi * si)
            numer_imag = total(qr * si - qi * sr)
            denom = total(qr * qr + qi * qi) + 2e-6
            live = (lane * 0 + limit) > k
            ar = jnp.where(live, jnp.broadcast_to(numer_real / denom, shape), 0.0)
            ai = jnp.where(live, jnp.broadcast_to(numer_imag / denom, shape), 0.0)
            e_ref[0] += ar * sr - ai * si
            e_ref[1] += ar * si + ai * sr
            s_ref[0] = sr - (ar * qr - ai * qi)
            s_ref[1] = si - (ar * qi + ai * qr)
            for n in range(2):
                a_ref[n, 0] -= ar * ahead_r[n] - ai * ahead_i[n]
                a_ref[n, 1] -= ar * ahead_i[n] + ai * ahead_r[n]
            for n, (vr, vi) in enumerate((back0, back2)):
                acc[n, 0] += ar * vr - ai * vi
                acc[n, 1] += ar * vi + ai * vr
            return carry

        lax.fori_loop(0, MR_MAX, step, 0)

        er, ei = e_ref[0], e_ref[1]
        bz = [-jnp.where(first, roll(acc[0, c], half), acc[0, c]) for c in range(2)]
        bt = [-jnp.where(first, acc[1, c], roll(acc[1, c], half)) for c in range(2)]
        packed = jnp.where(low, er, ei)
        sbuf[ph, 0] = jnp.where(h_is_0, packed, jnp.where(low, bt[0], bt[1]))
        sbuf[ph, 1] = packed
        sbuf[ph, 2] = jnp.where(low, bz[0], bz[1])

        @pl.when(ph == 0)
        def _():
            pl.semaphore_wait(barrier, 4)

        target = lax.rem(ta + nt + 2 * h - 1, nt)
        sends = []
        for n, where_to in enumerate(({"ta": target}, {"sa": z_prev}, {"sa": z_next})):
            send = pltpu.make_async_remote_copy(
                src_ref=sbuf.at[ph, n],
                dst_ref=rbuf.at[ph, n],
                send_sem=ssem.at[ph, n],
                recv_sem=rsem.at[ph, n],
                device_id=where_to,
                device_id_type=MESH,
            )
            send.start()
            sends.append(send)

        for c, ec in enumerate((er, ei)):
            xs[h, c] += ec
            rs[h, c] = s_ref[c]

        def unpack(n):
            m = rbuf[ph, n]
            w = roll(m, half)
            return jnp.where(low, m, w), jnp.where(low, w, m)

        sends[1].wait()
        sends[2].wait()
        got_e, got_b = unpack(1), unpack(2)

        def hop(times):
            inputs = []
            for c in range(2):
                zin = jnp.where(z_last, roll(got_e[c], -plane), 0.0)
                inputs.append(jnp.where(first, zin, times[c]))
            sweep_matrices(3, other, inputs, None, None, False)
            for c in range(2):
                u = gathered(c)
                zb = jnp.where(z_first, roll(got_b[c], plane), 0.0)
                rs[other, c] += u + roll(u, half) + zb

        @pl.when(h == 0)
        def _():
            for c in range(2):
                rs[1, c] += bt[c]
            sends[0].wait()
            hop(unpack(0))

        @pl.when(h == 1)
        def _():
            hop((er, ei))
            sends[0].wait()
            got_t = unpack(0)
            for c in range(2):
                rs[0, c] += got_t[c]

        return token

    lax.fori_loop(0, PHASES, phase, 0)

    for c in range(2):
        x_ref[c] = jnp.where(low, xs[0, c], xs[1, c])
        r_ref[c] = jnp.where(low, rs[0, c], rs[1, c])


def shards(nt, nz, rhs, links, clover, mr_steps):
    dof, lanes = rhs.shape[2], rhs.shape[-1]
    f32 = jnp.float32
    vmem = pl.BlockSpec(memory_space=pltpu.VMEM)
    hbm = pl.BlockSpec(memory_space=pltpu.HBM)
    x, r = pl.pallas_call(
        functools.partial(kernel, nt, nz),
        out_shape=[jax.ShapeDtypeStruct((2, dof, lanes), f32)] * 2,
        in_specs=[hbm, hbm, hbm, hbm],
        out_specs=[vmem, vmem],
        scratch_shapes=[
            pltpu.VMEM((2, dof, lanes), f32),
            pltpu.SMEM((2,), jnp.int32),
            pltpu.VMEM((4, 2, dof, dof, lanes), jnp.bfloat16),
            pltpu.VMEM((2, dof, dof, lanes), jnp.bfloat16),
            pltpu.VMEM((4, 2, 2, dof, dof, lanes), f32),
            pltpu.VMEM((2, 2, dof, lanes), f32),
            pltpu.VMEM((2, 2, dof, lanes), f32),
            pltpu.VMEM((2, dof, lanes), f32),
            pltpu.VMEM((2, dof, lanes), f32),
            pltpu.VMEM((2, 2, dof, lanes), f32),
            pltpu.VMEM((2, 2, dof, lanes), f32),
            pltpu.VMEM((3, dof, lanes), f32),
            pltpu.VMEM((2, 8 * dof, lanes), f32),
            pltpu.VMEM((PHASES, 3, dof, lanes), f32),
            pltpu.VMEM((PHASES, 3, dof, lanes), f32),
            pltpu.SemaphoreType.DMA((7,)),
            pltpu.SemaphoreType.DMA((PHASES, 3)),
            pltpu.SemaphoreType.DMA((PHASES, 3)),
        ],
        compiler_params=pltpu.CompilerParams(
            collective_id=0, has_side_effects=True, vmem_limit_bytes=67043328
        ),
    )(
        rhs.reshape(2, dof, lanes),
        links.reshape(4, 2, dof, dof, lanes),
        clover.reshape(2, dof, dof, lanes),
        mr_steps.reshape(2),
    )
    return x.reshape(rhs.shape), r.reshape(rhs.shape)


def solution(mesh):
    placed = (
        P(None, None, None, "ta", "sa", None),
        P(None, None, None, None, "ta", "sa", None),
        P(None, None, None, "ta", "sa", None),
        P("ta", "sa", None),
    )
    return jax.shard_map(
        functools.partial(shards, mesh.shape["ta"], mesh.shape["sa"]),
        mesh=mesh,
        in_specs=placed,
        out_specs=(P(None, None, None, "ta", "sa", None), P(None, None, None, "ta", "sa", None)),
        check_vma=False,
    )
```

```python
import functools

import jax
import jax.numpy as jnp
from jax import lax
from jax.experimental import pallas as pl
from jax.experimental.pallas import tpu as pltpu
from jax.sharding import PartitionSpec as P

LZ = 4
LY = 4
LX = 4
MR_MAX = 3
SWEEPS = 2
PHASES = 2 * SWEEPS
UNROLL = 10
PREPARE_UNROLL = 8
MESH = pl.DeviceIdType.MESH


def kernel(
    nt,
    nz,
    rhs_hbm,
    links_ref,
    clover_ref,
    steps_hbm,
    x_ref,
    r_ref,
    rhs_ref,
    steps_ref,
    lk,
    cl,
    g,
    rs,
    xs,
    s_ref,
    e_ref,
    acc,
    a_ref,
    gv,
    f_ref,
    sbuf,
    rbuf,
    csem,
    ssem,
    rsem,
):
    dof, lanes = rhs_ref.shape[1:]
    half = lanes // 2
    tiles = dof // 8
    ta = lax.axis_index("ta")
    sa = lax.axis_index("sa")
    t_next, t_prev = lax.rem(ta + 1, nt), lax.rem(ta + nt - 1, nt)
    z_next, z_prev = lax.rem(sa + 1, nz), lax.rem(sa + nz - 1, nz)

    copies = [
        pltpu.make_async_copy(links_ref.at[d], lk.at[d], csem.at[d]) for d in range(4)
    ] + [
        pltpu.make_async_copy(clover_ref, cl, csem.at[4]),
        pltpu.make_async_copy(rhs_hbm, rhs_ref, csem.at[5]),
        pltpu.make_async_copy(steps_hbm, steps_ref, csem.at[6]),
    ]
    for d in (5, 1, 2, 0, 3, 4, 6):
        copies[d].start()

    barrier = pltpu.get_barrier_semaphore()
    for where_to in ({"ta": t_next}, {"ta": t_prev}, {"sa": z_next}, {"sa": z_prev}):
        pl.semaphore_signal(barrier, inc=1, device_id=where_to, device_id_type=MESH)

    shape = (dof, lanes)
    lane = lax.broadcasted_iota(jnp.int32, shape, 1)
    row = lax.broadcasted_iota(jnp.int32, shape, 0)
    signs = jnp.where(row < dof // 2, 1.0, -1.0).astype(jnp.float32)
    low = lane < half
    site = lane % half
    zpos = site // (LY * LX)
    ypos = site // LX % LY
    xpos = site % LX
    z_last, z_first = zpos == LZ - 1, zpos == 0
    y_last, y_first = ypos == LY - 1, ypos == 0
    x_last, x_first = xpos == LX - 1, xpos == 0
    zero = jnp.zeros(shape, jnp.float32)
    plane = LY * LX

    def roll(v, by):
        return pltpu.roll(v, by % lanes, 1)

    copies[5].wait()
    for c in range(2):
        v = rhs_ref[c]
        w = roll(v, half)
        rs[0, c] = jnp.where(low, v, w)
        rs[1, c] = jnp.where(low, w, v)
        xs[0, c] = zero
        xs[1, c] = zero

    def prepare(plain, rolled, groups):
        def body(outer, carry):
            for inner in range(PREPARE_UNROLL):
                i = outer * PREPARE_UNROLL + inner
                for c in range(2):
                    b = roll(rolled(c, i).astype(jnp.float32), half)
                    for source, group in zip(plain, groups):
                        a = source(c, i).astype(jnp.float32)
                        g[group, 0, c, i] = jnp.where(low, a, b)
                        g[group, 1, c, i] = jnp.where(low, b, a)
            return carry

        lax.fori_loop(0, dof // PREPARE_UNROLL, body, 0)

    def link(d):
        return lambda c, i: lk[d, c, i]

    for d in (1, 2, 0):
        copies[d].wait()
    prepare([link(2), link(0)], link(1), [0, 3])
    for d in (3, 4, 6):
        copies[d].wait()
    prepare([lambda c, i: cl[c, i], link(0)], link(3), [1, 2])

    def fold(v):
        total = v[0:8]
        for t in range(1, tiles):
            total = total + v[8 * t : 8 * t + 8]
        return total

    def gathered(slot):
        parts = []
        for t in range(tiles):
            total = None
            for k in range(8):
                piece = f_ref[slot, pl.ds(8 * 8 * t + k, 8, stride=8), :]
                total = piece if total is None else total + piece
            parts.append(total)
        return jnp.concatenate(parts, axis=0)

    def sweep_matrices(forward, forward_half, inputs, backward, backward_half, more):
        vr, vi = inputs
        vs = vr + vi
        shared = backward == forward

        def one(i, carry):
            mr, mi = g[forward, forward_half, 0, i], g[forward, forward_half, 1, i]
            ms = mr + mi
            p1 = fold(mr * vr)
            p2 = fold(mi * vi)
            p3 = fold(ms * vs)
            at = pl.multiple_of(8 * i, 8)
            real_part, imag_part = p1 - p2, p3 - p1 - p2
            if more:
                real_part = real_part + f_ref[0, pl.ds(at, 8), :]
                imag_part = imag_part + f_ref[1, pl.ds(at, 8), :]
            f_ref[0, pl.ds(at, 8), :] = real_part
            f_ref[1, pl.ds(at, 8), :] = imag_part
            if backward is None:
                return carry
            if not shared:
                mr, mi = g[backward, backward_half, 0, i], g[backward, backward_half, 1, i]
                ms = mr + mi
            b1, b2, b3 = carry
            br = gv[0, pl.ds(i, 1), :]
            bi = gv[1, pl.ds(i, 1), :]
            bd = gv[2, pl.ds(i, 1), :]
            return (b1 + mr * br, b2 + mi * bi, b3 + ms * bd)

        def body(outer, carry):
            for inner in range(UNROLL):
                carry = one(outer * UNROLL + inner, carry)
            return carry

        start = 0 if backward is None else (zero, zero, zero)
        got = lax.fori_loop(0, dof // UNROLL, body, start)
        if backward is None:
            return None
        b1, b2, b3 = got
        return -signs * (b1 + b2), -signs * (b1 - b2 - b3)

    def phase(ph, token):
        h = lax.rem(ph + sa, 2)
        other = 1 - h
        limit = steps_ref[h]
        first = (lane // half) == h
        h_is_0 = (lane * 0 + h) == 0

        def ahead(v):
            n = -v
            ya = jnp.where(y_last, roll(n, (LY - 1) * LX), roll(n, -LX))
            za = jnp.where(z_last, 0.0, roll(n, -plane))
            xa = jnp.where(x_last, roll(n, LX - 1), roll(n, -1))
            return jnp.where(first, ya, za), jnp.where(first, v, xa)

        for c in range(2):
            v = rs[h, c]
            s_ref[c] = v
            e_ref[c] = zero
            acc[0, c] = zero
            acc[1, c] = zero
            a_ref[0, c], a_ref[1, c] = ahead(v)

        def images():
            sr, si = s_ref[0], s_ref[1]
            gr, gi = signs * sr, signs * si
            gv[0] = gr
            gv[1] = gi
            gv[2] = gr - gi
            back0 = sweep_matrices(0, h, (a_ref[0, 0], a_ref[0, 1]), 0, h, False)
            back2 = sweep_matrices(1, h, (a_ref[1, 0], a_ref[1, 1]), 2, h, True)
            q = []
            for c in range(2):
                b, d = back0[c], back2[c]
                yb = jnp.where(y_first, roll(b, -(LY - 1) * LX), roll(b, LX))
                zb = jnp.where(z_first, 0.0, roll(b, plane))
                xb = jnp.where(x_first, roll(d, -(LX - 1)), roll(d, 1))
                u = gathered(c) + jnp.where(first, yb, zb) + jnp.where(first, 0.0, xb)
                q.append(u + roll(u, half))
            qr, qi = q
            ahead_r, ahead_i = ahead(qr), ahead(qi)
            return sr, si, qr, qi, ahead_r, ahead_i, back0, back2

        def total(v):
            return jnp.sum(jnp.sum(fold(v), axis=0, keepdims=True), axis=1, keepdims=True)

        def scale(k, sr, si, qr, qi):
            numer_real = total(qr * sr + qi * si)
            numer_imag = total(qr * si - qi * sr)
            denom = total(qr * qr + qi * qi) + 2e-6
            live = (lane * 0 + limit) > k
            ar = jnp.where(live, jnp.broadcast_to(numer_real / denom, shape), 0.0)
            ai = jnp.where(live, jnp.broadcast_to(numer_imag / denom, shape), 0.0)
            return ar, ai

        def times(ar, ai, v):
            return ar * v[0] - ai * v[1], ar * v[1] + ai * v[0]

        def step(k, carry):
            sr, si, qr, qi, ahead_r, ahead_i, back0, back2 = images()
            ar, ai = scale(k, sr, si, qr, qi)
            es = times(ar, ai, (sr, si))
            qs = times(ar, ai, (qr, qi))
            for c, old in enumerate((sr, si)):
                e_ref[c] += es[c]
                s_ref[c] = old - qs[c]
            for n, back in enumerate((back0, back2)):
                moved = times(ar, ai, (ahead_r[n], ahead_i[n]))
                added = times(ar, ai, back)
                for c in range(2):
                    a_ref[n, c] -= moved[c]
                    acc[n, c] += added[c]
            return carry

        lax.fori_loop(0, MR_MAX - 1, step, 0)

        def pack(v):
            return jnp.where(low, v[0], v[1])

        def bt_of(v):
            return [-jnp.where(first, v[c], roll(v[c], half)) for c in range(2)]

        def sender(n, where_to, src, dst):
            return pltpu.make_async_remote_copy(
                src_ref=src,
                dst_ref=dst,
                send_sem=ssem.at[ph, n],
                recv_sem=rsem.at[ph, n],
                device_id=where_to,
                device_id_type=MESH,
            )

        target = {"ta": lax.rem(ta + nt + 2 * h - 1, nt)}
        e_old = (e_ref[0], e_ref[1])

        @pl.when(ph == 0)
        def _():
            pl.semaphore_wait(barrier, 4)

        sr, si, qr, qi, _, _, back0, back2 = images()
        ar, ai = scale(MR_MAX - 1, sr, si, qr, qi)
        es = times(ar, ai, (sr, si))
        e_new = [e_old[c] + es[c] for c in range(2)]
        added = times(ar, ai, back2)
        bt = bt_of([acc[1, c] + added[c] for c in range(2)])
        sbuf[ph, 0] = jnp.where(h_is_0, pack(e_new), pack(bt))
        sends = [sender(0, target, sbuf.at[ph, 0], rbuf.at[ph, 0])]
        sends[0].start()
        bs = times(ar, ai, back0)
        bz = []
        for c in range(2):
            v = acc[0, c] + bs[c]
            bz.append(-jnp.where(first, roll(v, half), v))
        sbuf[ph, 1] = pack(e_new)
        sbuf[ph, 2] = pack(bz)
        sends.append(sender(1, {"sa": z_prev}, sbuf.at[ph, 1], rbuf.at[ph, 1]))
        sends.append(sender(2, {"sa": z_next}, sbuf.at[ph, 2], rbuf.at[ph, 2]))
        sends[1].start()
        sends[2].start()

        qs = times(ar, ai, (qr, qi))
        for c, old in enumerate((sr, si)):
            xs[h, c] += e_new[c]
            rs[h, c] = old - qs[c]

        def unpack(n):
            m = rbuf[ph, n]
            w = roll(m, half)
            return jnp.where(low, m, w), jnp.where(low, w, m)

        sends[1].wait()
        sends[2].wait()
        got_e, got_b = unpack(1), unpack(2)

        def hop(times):
            inputs = []
            for c in range(2):
                zin = jnp.where(z_last, roll(got_e[c], -plane), 0.0)
                inputs.append(jnp.where(first, zin, times[c]))
            sweep_matrices(3, other, inputs, None, None, False)
            for c in range(2):
                u = gathered(c)
                zb = jnp.where(z_first, roll(got_b[c], plane), 0.0)
                rs[other, c] += u + roll(u, half) + zb

        @pl.when(h == 0)
        def _():
            for c in range(2):
                rs[1, c] += bt[c]
            sends[0].wait()
            hop(unpack(0))

        @pl.when(h == 1)
        def _():
            hop(e_new)
            sends[0].wait()
            got_t = unpack(0)
            for c in range(2):
                rs[0, c] += got_t[c]

        return token

    lax.fori_loop(0, PHASES, phase, 0)

    for c in range(2):
        x_ref[c] = jnp.where(low, xs[0, c], xs[1, c])
        r_ref[c] = jnp.where(low, rs[0, c], rs[1, c])


def shards(nt, nz, rhs, links, clover, mr_steps):
    dof, lanes = rhs.shape[2], rhs.shape[-1]
    f32 = jnp.float32
    vmem = pl.BlockSpec(memory_space=pltpu.VMEM)
    hbm = pl.BlockSpec(memory_space=pltpu.HBM)
    x, r = pl.pallas_call(
        functools.partial(kernel, nt, nz),
        out_shape=[jax.ShapeDtypeStruct((2, dof, lanes), f32)] * 2,
        in_specs=[hbm, hbm, hbm, hbm],
        out_specs=[vmem, vmem],
        scratch_shapes=[
            pltpu.VMEM((2, dof, lanes), f32),
            pltpu.SMEM((2,), jnp.int32),
            pltpu.VMEM((4, 2, dof, dof, lanes), jnp.bfloat16),
            pltpu.VMEM((2, dof, dof, lanes), jnp.bfloat16),
            pltpu.VMEM((4, 2, 2, dof, dof, lanes), f32),
            pltpu.VMEM((2, 2, dof, lanes), f32),
            pltpu.VMEM((2, 2, dof, lanes), f32),
            pltpu.VMEM((2, dof, lanes), f32),
            pltpu.VMEM((2, dof, lanes), f32),
            pltpu.VMEM((2, 2, dof, lanes), f32),
            pltpu.VMEM((2, 2, dof, lanes), f32),
            pltpu.VMEM((3, dof, lanes), f32),
            pltpu.VMEM((2, 8 * dof, lanes), f32),
            pltpu.VMEM((PHASES, 3, dof, lanes), f32),
            pltpu.VMEM((PHASES, 3, dof, lanes), f32),
            pltpu.SemaphoreType.DMA((7,)),
            pltpu.SemaphoreType.DMA((PHASES, 3)),
            pltpu.SemaphoreType.DMA((PHASES, 3)),
        ],
        compiler_params=pltpu.CompilerParams(
            collective_id=0, has_side_effects=True, vmem_limit_bytes=67043328
        ),
    )(
        rhs.reshape(2, dof, lanes),
        links.reshape(4, 2, dof, dof, lanes),
        clover.reshape(2, dof, dof, lanes),
        mr_steps.reshape(2),
    )
    return x.reshape(rhs.shape), r.reshape(rhs.shape)


def solution(mesh):
    placed = (
        P(None, None, None, "ta", "sa", None),
        P(None, None, None, None, "ta", "sa", None),
        P(None, None, None, "ta", "sa", None),
        P("ta", "sa", None),
    )
    return jax.shard_map(
        functools.partial(shards, mesh.shape["ta"], mesh.shape["sa"]),
        mesh=mesh,
        in_specs=placed,
        out_specs=(P(None, None, None, "ta", "sa", None), P(None, None, None, "ta", "sa", None)),
        check_vma=False,
    )
```
